32 devices in a mesh: ia: 4 (over z), ja: 2 (over core), ka: 4 (over y, x).
Axes of the slice: x: 2, y: 2, z: 4, core: 2. Of those that a mesh axis runs over, the one named last changes fastest.
Arguments:
- attended: bfloat16 [1024, 8192], P('ia', ('ja', 'ka')), may hold values from -6 to 6
- out_weight: bfloat16 [8192, 8192], P(('ja', 'ia'), 'ka'), may hold values from -0.0625 to 0.0625
- cotangent: bfloat16 [1024, 8192], P('ia', ('ka', 'ja')), may hold values from -3 to 3
Outputs:
- projected: bfloat16 [1024, 8192], P('ia', ('ka', 'ja'))
- input_grad: bfloat16 [1024, 8192], P('ia', ('ja', 'ka'))
- weight_grad: bfloat16 [8192, 8192], P(('ja', 'ia'), 'ka')
The draws below stay inside these ranges and needn't reach their ends.
All inputs are finite; a program needn't handle non-finite values.
Results may differ from the reference program's by a relative error of at most 0.015.
Values may be sent and summed in bfloat16 or wider, within the bound.
A program may use at most 128 MiB of HBM per device.

```python
import jax
import jax.numpy as jnp
from jax import lax

D = 8192
TOK_ROW = 256
TOKENS = 1024
N_IA = 4


def levels(key, dims, cuts, smallest, top_value):
    level, own = 1.0, jax.random.fold_in(key, 6)
    for dim, shards_of in cuts:
        heights = jnp.exp(jax.random.uniform(jax.random.fold_in(own, dim), (shards_of,), jnp.float32, smallest / len(cuts), top_value / len(cuts)))
        level = level * jnp.repeat(heights, dims[dim] // shards_of).reshape([-1 if axis == dim else 1 for axis in range(len(dims))])
    return level


def centred(key, extent, deviation, most, cuts=(), held_as=jnp.bfloat16):
    array = deviation * jax.random.normal(key, extent, jnp.float32)
    if cuts:
        array = array * levels(key, extent, cuts, -0.22, 0.18)
    return jnp.clip(array, -most, most).astype(held_as)


def setup_inputs(seed: int = 0) -> dict:
    key_list = jax.random.split(jax.random.key(seed), 4)
    attended = centred(key_list[0], (TOKENS, D), 1.0, 6.0, ((0, 4), (1, 8)))
    out_weight = centred(key_list[1], (D, D), D ** -0.5, 0.0625, ((0, 8), (1, 4)))
    cotangent = centred(key_list[2], (TOKENS, D), 0.5, 3.0, ((0, 4), (1, 8)))
    return {"attended": attended, "out_weight": out_weight, "cotangent": cotangent}


def reference(attended, out_weight, cotangent):
    projected = jnp.dot(attended, out_weight, preferred_element_type=jnp.float32).astype(jnp.bfloat16)
    input_grad = lax.dot_general(cotangent, out_weight, (((1,), (1,)), ((), ())), preferred_element_type=jnp.float32).astype(jnp.bfloat16)
    head_blocks = attended.reshape(N_IA, TOK_ROW, D)
    grad_blocks = cotangent.reshape(N_IA, TOK_ROW, D)

    def accumulate(total, pair):
        partial_value = lax.dot_general(pair[0], pair[1], (((0,), (0,)), ((), ())), preferred_element_type=jnp.float32)
        return total + partial_value.astype(jnp.bfloat16).astype(jnp.float32), None

    weight_sum, unused = lax.scan(accumulate, jnp.zeros((D, D), jnp.float32), (head_blocks, grad_blocks))
    return projected, input_grad, weight_sum.astype(jnp.bfloat16)
```

```python
import functools

import jax
import jax.numpy as jnp
from jax import lax
from jax.experimental import pallas as pl
from jax.experimental.pallas import tpu as pltpu
from jax.sharding import PartitionSpec as P

MESH = pl.DeviceIdType.MESH
VMEM_LIMIT = 60 * 1024 * 1024


def gathered_weight(attended, out_weight, cotangent):
    head_rows = lax.all_gather(attended, "ka", axis=1, tiled=True)
    weight_local = lax.all_gather(out_weight, "ia", axis=0, tiled=True)
    partial_value = jnp.dot(head_rows, weight_local, preferred_element_type=jnp.float32)
    projected = lax.psum_scatter(
        partial_value.astype(jnp.bfloat16), "ja", scatter_dimension=1, tiled=True
    )
    grad_rows = lax.all_gather(cotangent, "ja", axis=1, tiled=True)
    input_terms = lax.dot_general(
        grad_rows, weight_local, (((1,), (1,)), ((), ())), preferred_element_type=jnp.float32
    )
    input_grad = lax.psum_scatter(
        input_terms.astype(jnp.bfloat16), "ka", scatter_dimension=1, tiled=True
    )
    weight_terms = lax.dot_general(
        head_rows, grad_rows, (((0,), (0,)), ((), ())), preferred_element_type=jnp.float32
    )
    weight_grad = lax.psum_scatter(
        weight_terms.astype(jnp.bfloat16), "ia", scatter_dimension=0, tiled=True
    )
    return projected, input_grad, weight_grad


def kernel(
    n, att, w_hbm, cot, proj, ig, wg,
    w, a_x, a_g, c_g, p_send, p_recv, p_own, z_buf, z_up, z_dn,
    i_part, i_recv, i_red, i_z, i_out,
    loc, sa, ra, sb, rb_, sc, rc, su, ru, sd, rd, spu, rpu, spd, rpd, spo, rpo,
    sp, rp, sru, rru, srd, rrd, si, ri, sz, rz, so, ro,
):
    ia, ja, ka = lax.axis_index("ia"), lax.axis_index("ja"), lax.axis_index("ka")
    other = 1 - ja
    tok, head = att.shape
    quart = tok // n
    half = cot.shape[1]
    rows_w = w.shape[0]
    f32, bf16 = jnp.float32, jnp.bfloat16

    def plus(x, r):
        return lax.rem(x + r, n)

    def minus(x, r):
        return lax.rem(x + n - r, n)

    def span(t):
        return pl.ds(pl.multiple_of(t * tok, tok), tok)

    def piece(t, q):
        return pl.ds(pl.multiple_of(t * tok + q * quart, quart), quart)

    def remote(src, dst, s, r, where):
        return pltpu.make_async_remote_copy(
            src_ref=src, dst_ref=dst, send_sem=s, recv_sem=r,
            device_id=where, device_id_type=MESH,
        )

    barrier = pltpu.get_barrier_semaphore()
    for r in range(1, n):
        pl.semaphore_signal(barrier, inc=1, device_id={"ka": plus(ka, r)}, device_id_type=MESH)
        pl.semaphore_signal(barrier, inc=1, device_id={"ia": plus(ia, r)}, device_id_type=MESH)
    pl.semaphore_signal(barrier, inc=1, device_id={"ja": other}, device_id_type=MESH)
    pl.semaphore_wait(barrier, 2 * (n - 1) + 1)

    def a_plane(r):
        q = plus(ka, r)
        return remote(att.at[pl.ds(pl.multiple_of(q * quart, quart), quart)], a_x.at[ka],
                      sa.at[r - 1], ra.at[r - 1], {"ka": q})

    def a_z(r):
        z = plus(ia, r)
        return remote(a_x.at[z], a_g.at[piece(ia, ka)], sb.at[r - 1], rb_.at[r - 1], {"ia": z})

    def a_spread(b, r):
        rows = a_g.at[piece(minus(ia, b), ka)]
        return remote(rows, rows, sc.at[b, r - 1], rc.at[b, r - 1], {"ka": plus(ka, r)})

    def c_up(d):
        block = c_g.at[ja, span(ia - (d - 1))]
        src = cot if d == 1 else block
        return remote(src, block, su.at[d - 1], ru.at[d - 1], {"ia": ia + 1})

    def c_down(d):
        block = c_g.at[ja, span(ia + (d - 1))]
        src = cot if d == 1 else block
        return remote(src, block, sd.at[d - 1], rd.at[d - 1], {"ia": ia - 1})

    def c_pair_up(d):
        block = c_g.at[ja, span(ia - d)]
        return remote(block, block, spu.at[d - 1], rpu.at[d - 1], {"ja": other})

    def c_pair_down(d):
        block = c_g.at[ja, span(ia + d)]
        return remote(block, block, spd.at[d - 1], rpd.at[d - 1], {"ja": other})

    c_pair_own = remote(cot, c_g.at[ja, span(ia)], spo.at[0], rpo.at[0], {"ja": other})

    def up_exists(d):
        return jnp.logical_and(ia + 1 < n, ia - (d - 1) >= 0)

    def down_exists(d):
        return jnp.logical_and(ia - 1 >= 0, ia + (d - 1) < n)

    def c_step(d):
        @pl.when(ia - d >= 0)
        def _():
            c_up(d).wait_recv()
            if d + 1 < n:
                @pl.when(ia + 1 < n)
                def _():
                    c_up(d + 1).start()
            c_pair_up(d).start()

        @pl.when(ia + d < n)
        def _():
            c_down(d).wait_recv()
            if d + 1 < n:
                @pl.when(ia - 1 >= 0)
                def _():
                    c_down(d + 1).start()
            c_pair_down(d).start()

    w_copy = pltpu.make_async_copy(w_hbm, w, loc.at[0])
    own_x = pltpu.make_async_copy(
        att.at[pl.ds(pl.multiple_of(ka * quart, quart), quart)], a_x.at[ka], loc.at[1])
    own_c = pltpu.make_async_copy(cot, c_g.at[ja, span(ia)], loc.at[2])
    own_a = pltpu.make_async_copy(a_x.at[ia], a_g.at[piece(ia, ka)], loc.at[3])
    for r in range(1, n):
        a_plane(r).start()
    own_x.start()

    @pl.when(up_exists(1))
    def _():
        c_up(1).start()

    @pl.when(down_exists(1))
    def _():
        c_down(1).start()

    c_pair_own.start()
    own_c.start()
    w_copy.start()
    own_x.wait()
    for r in range(1, n):
        a_plane(r).wait_recv()
    for r in range(1, n):
        a_z(r).start()
    own_a.start()
    own_a.wait()
    for r in range(1, n):
        a_spread(0, r).start()
    c_step(1)
    for b in range(1, n):
        a_z(b).wait_recv()
        for r in range(1, n):
            a_spread(b, r).start()
    for d in range(2, n - 1):
        c_step(d)
    for b in range(n):
        for r in range(1, n):
            a_spread(b, r).wait_recv()
    w_copy.wait()

    width = 256

    def project(which, out):
        @pl.loop(0, half // width)
        def _(c):
            at = pl.multiple_of(which * half + c * width, width)
            to = pl.multiple_of(c * width, width)
            out[:, pl.ds(to, width)] = jnp.dot(
                a_g[...], w[:, pl.ds(at, width)], preferred_element_type=f32
            ).astype(out.dtype)

    def pair(t):
        return remote(p_send.at[pl.ds(t * tok, tok)], p_recv.at[pl.ds(t * tok, tok)],
                      sp.at[t], rp.at[t], {"ja": other})

    project(other, p_send)
    for t in range(n):
        pair(t).start()
    project(ja, p_own)
    for t in range(n):
        pair(t).wait_recv()

    step_rows = 32

    def add_block(d, out, *incoming):
        @pl.loop(0, tok // step_rows)
        def _(i):
            at = pl.multiple_of(i * step_rows, step_rows)
            mine = pl.ds(d * tok + at, step_rows)
            here = pl.ds(at, step_rows)
            total = p_own[mine, :] + p_recv[mine, :].astype(f32)
            for ref in incoming:
                total = total + ref[here, :].astype(f32)
            out[here, :] = total.astype(bf16)

    def r_up(d):
        return remote(z_buf.at[d], z_up.at[d], sru.at[d], rru.at[d], {"ia": ia + 1})

    def r_down(d):
        return remote(z_buf.at[d], z_dn.at[d], srd.at[d], rrd.at[d], {"ia": ia - 1})

    def reduce_step(tau):
        for m in range(n):
            @pl.when(ia == m)
            def _():
                d = n - 1 - (tau - m)
                if 0 <= tau - m and d > m:
                    if m > 0:
                        r_up(d).wait_recv()
                        add_block(d, z_buf.at[d], z_up.at[d])
                    else:
                        add_block(d, z_buf.at[d])
                    r_up(d).start()
                d = tau - (n - 1 - m)
                if 0 <= d < m:
                    if m < n - 1:
                        r_down(d).wait_recv()
                        add_block(d, z_buf.at[d], z_dn.at[d])
                    else:
                        add_block(d, z_buf.at[d])
                    r_down(d).start()

    reduce_step(0)

    c_step(n - 1)
    own_c.wait()
    c_pair_own.wait_recv()
    for d in range(1, n):
        @pl.when(ia - d >= 0)
        def _():
            c_pair_up(d).wait_recv()

        @pl.when(ia + d < n)
        def _():
            c_pair_down(d).wait_recv()

    @pl.loop(0, rows_w // width)
    def _(c):
        at = pl.multiple_of(c * width, width)
        total = lax.dot_general(
            c_g[0], w[pl.ds(at, width), :half], (((1,), (1,)), ((), ())),
            preferred_element_type=f32)
        total = total + lax.dot_general(
            c_g[1], w[pl.ds(at, width), half:], (((1,), (1,)), ((), ())),
            preferred_element_type=f32)
        i_part[:, pl.ds(at, width)] = total.astype(bf16)

    def i_plane(b, r):
        q = plus(ka, r)
        t = plus(ia, b)
        return remote(i_part.at[piece(t, q)], i_recv.at[b, r - 1],
                      si.at[b, r - 1], ri.at[b, r - 1], {"ka": q})

    def i_to_z(b):
        return remote(i_red.at[b], i_z.at[ia], sz.at[b - 1], rz.at[b - 1], {"ia": plus(ia, b)})

    def i_back(r):
        k = plus(ka, r)
        return remote(i_z.at[k], i_out.at[pl.ds(pl.multiple_of(ka * quart, quart), quart)],
                      so.at[r - 1], ro.at[r - 1], {"ka": k})

    order = list(range(1, n)) + [0]
    for b in order:
        for r in range(1, n):
            i_plane(b, r).start()

    chunks = head // width

    def weight_chunks(first, last):
        @pl.loop(first, last)
        def _(c):
            at = pl.multiple_of(c * width, width)
            lhs = a_g[:, pl.ds(at, width)]
            for j in range(2):
                wg[pl.ds(at, width), j * half:(j + 1) * half] = lax.dot_general(
                    lhs, c_g[j], (((0,), (0,)), ((), ())), preferred_element_type=f32
                ).astype(bf16)

    weight_chunks(0, chunks // 2)
    reduce_step(1)
    for b in order:
        for r in range(1, n):
            i_plane(b, r).wait_recv()
        total = i_part[piece(plus(ia, b), ka), :].astype(f32)
        for r in range(1, n):
            total = total + i_recv[b, r - 1].astype(f32)
        if b == 0:
            i_z[ia] = total.astype(bf16)
        else:
            i_red[b] = total.astype(bf16)
            i_to_z(b).start()
    for tau in range(2, n - 1):
        reduce_step(tau)
    weight_chunks(chunks // 2, chunks)
    for b in range(1, n):
        i_to_z(b).wait_recv()
    for r in range(1, n):
        i_back(r).start()
    ig[pl.ds(pl.multiple_of(ka * quart, quart), quart), :] = i_z[ka]
    for m in range(n):
        @pl.when(ia == m)
        def _():
            incoming = []
            if m > 0:
                r_up(m).wait_recv()
                incoming.append(z_up.at[m])
            if m < n - 1:
                r_down(m).wait_recv()
                incoming.append(z_dn.at[m])
            add_block(m, proj, *incoming)
    for r in range(1, n):
        i_back(r).wait_recv()
        rows = pl.ds(pl.multiple_of(minus(ka, r) * quart, quart), quart)
        ig[rows, :] = i_out[rows, :]

    for r in range(1, n):
        a_plane(r).wait_send()
        a_z(r).wait_send()
        i_to_z(r).wait_send()
        i_back(r).wait_send()
        for b in range(n):
            a_spread(b, r).wait_send()
            i_plane(b, r).wait_send()
    c_pair_own.wait_send()
    for t in range(n):
        pair(t).wait_send()
    for d in range(1, n):
        @pl.when(up_exists(d))
        def _():
            c_up(d).wait_send()

        @pl.when(down_exists(d))
        def _():
            c_down(d).wait_send()

        @pl.when(ia - d >= 0)
        def _():
            c_pair_up(d).wait_send()

        @pl.when(ia + d < n)
        def _():
            c_pair_down(d).wait_send()

    for d in range(n):
        @pl.when(ia < d)
        def _():
            r_up(d).wait_send()

        @pl.when(ia > d)
        def _():
            r_down(d).wait_send()


def stationary_weight(n, attended, out_weight, cotangent):
    tok, head = attended.shape
    half = cotangent.shape[1]
    rows = n * tok
    quart = tok // n
    bf16, f32 = jnp.bfloat16, jnp.float32
    vmem = pl.BlockSpec(memory_space=pltpu.VMEM)
    dma = pltpu.SemaphoreType.DMA
    one = dma((n - 1,))
    two = dma((n, n - 1))
    full = dma((n,))
    flops = 6 * rows * out_weight.shape[0] * out_weight.shape[1]
    return pl.pallas_call(
        functools.partial(kernel, n),
        out_shape=(
            jax.ShapeDtypeStruct((tok, half), bf16),
            jax.ShapeDtypeStruct((tok, head), bf16),
            jax.ShapeDtypeStruct(out_weight.shape, bf16),
        ),
        in_specs=[vmem, pl.BlockSpec(memory_space=pl.ANY), vmem],
        out_specs=(vmem, vmem, vmem),
        scratch_shapes=[
            pltpu.VMEM(out_weight.shape, bf16),
            pltpu.VMEM((n, quart, head), bf16),
            pltpu.VMEM((rows, head), bf16),
            pltpu.VMEM((2, rows, half), bf16),
            pltpu.VMEM((rows, half), bf16),
            pltpu.VMEM((rows, half), bf16),
            pltpu.VMEM((rows, half), f32),
            pltpu.VMEM((n, tok, half), bf16),
            pltpu.VMEM((n, tok, half), bf16),
            pltpu.VMEM((n, tok, half), bf16),
            pltpu.VMEM((rows, head), bf16),
            pltpu.VMEM((n, n - 1, quart, head), bf16),
            pltpu.VMEM((n, quart, head), bf16),
            pltpu.VMEM((n, quart, head), bf16),
            pltpu.VMEM((tok, head), bf16),
            full, one, one, one, one, two, two, one, one, one, one,
            one, one, one, one, dma((1,)), dma((1,)),
            full, full, full, full, full, full, two, two, one, one, one, one,
        ],
        compiler_params=pltpu.CompilerParams(
            collective_id=0, has_side_effects=True, vmem_limit_bytes=VMEM_LIMIT
        ),
        cost_estimate=pl.CostEstimate(
            flops=flops, bytes_accessed=6 * rows * half, transcendentals=0
        ),
    )(attended, out_weight, cotangent)


def on_device(sizes, attended, out_weight, cotangent):
    tok, head = attended.shape
    half = cotangent.shape[1]
    n = sizes["ia"]
    tiles = tok % (16 * n) == 0 and head % 256 == 0 and half % 256 == 0
    fits = (
        sizes["ja"] == 2
        and sizes["ka"] == n
        and n >= 3
        and out_weight.shape == (head, 2 * half)
        and head % 512 == 0
        and 8 * out_weight.size + 2 * n * tok * (6 * head + 9 * half) < VMEM_LIMIT
    )
    if tiles and fits:
        return stationary_weight(n, attended, out_weight, cotangent)
    return gathered_weight(attended, out_weight, cotangent)


def solution(mesh):
    return jax.shard_map(
        functools.partial(on_device, dict(mesh.shape)),
        mesh=mesh,
        in_specs=(P("ia", ("ja", "ka")), P(("ja", "ia"), "ka"), P("ia", ("ka", "ja"))),
        out_specs=(P("ia", ("ka", "ja")), P("ia", ("ja", "ka")), P(("ja", "ia"), "ka")),
        check_vma=False,
    )
```

```python
import functools

import jax
import jax.numpy as jnp
from jax import lax
from jax.experimental import pallas as pl
from jax.experimental.pallas import tpu as pltpu
from jax.sharding import PartitionSpec as P

MESH = pl.DeviceIdType.MESH
VMEM_LIMIT = 44 * 1024 * 1024


def gathered_weight(attended, out_weight, cotangent):
    head_rows = lax.all_gather(attended, "ka", axis=1, tiled=True)
    weight_local = lax.all_gather(out_weight, "ia", axis=0, tiled=True)
    partial_value = jnp.dot(head_rows, weight_local, preferred_element_type=jnp.float32)
    projected = lax.psum_scatter(
        partial_value.astype(jnp.bfloat16), "ja", scatter_dimension=1, tiled=True
    )
    grad_rows = lax.all_gather(cotangent, "ja", axis=1, tiled=True)
    input_terms = lax.dot_general(
        grad_rows, weight_local, (((1,), (1,)), ((), ())), preferred_element_type=jnp.float32
    )
    input_grad = lax.psum_scatter(
        input_terms.astype(jnp.bfloat16), "ka", scatter_dimension=1, tiled=True
    )
    weight_terms = lax.dot_general(
        head_rows, grad_rows, (((0,), (0,)), ((), ())), preferred_element_type=jnp.float32
    )
    weight_grad = lax.psum_scatter(
        weight_terms.astype(jnp.bfloat16), "ia", scatter_dimension=0, tiled=True
    )
    return projected, input_grad, weight_grad


def kernel(
    n, att, w_hbm, cot, proj, ig, wg,
    w, a_x, a_g, c_g, p_send, p_recv, p_own, z_buf, z_up, z_dn,
    i_part, i_recv, i_red, i_z, i_out,
    loc, sa, ra, sb, rb_, sc, rc, su, ru, sd, rd, spu, rpu, spd, rpd, spo, rpo,
    sp, rp, sru, rru, srd, rrd, si, ri, sz, rz, so, ro,
):
    ia, ja, ka = lax.axis_index("ia"), lax.axis_index("ja"), lax.axis_index("ka")
    other = 1 - ja
    tok, head = att.shape
    quart = tok // n
    half = cot.shape[1]
    rows_w = w.shape[0]
    f32, bf16 = jnp.float32, jnp.bfloat16

    def plus(x, r):
        return lax.rem(x + r, n)

    def minus(x, r):
        return lax.rem(x + n - r, n)

    def span(t):
        return pl.ds(pl.multiple_of(t * tok, tok), tok)

    def piece(t, q):
        return pl.ds(pl.multiple_of(t * tok + q * quart, quart), quart)

    def remote(src, dst, s, r, where):
        return pltpu.make_async_remote_copy(
            src_ref=src, dst_ref=dst, send_sem=s, recv_sem=r,
            device_id=where, device_id_type=MESH,
        )

    barrier = pltpu.get_barrier_semaphore()
    for r in range(1, n):
        pl.semaphore_signal(barrier, inc=1, device_id={"ka": plus(ka, r)}, device_id_type=MESH)
        pl.semaphore_signal(barrier, inc=1, device_id={"ia": plus(ia, r)}, device_id_type=MESH)
    pl.semaphore_signal(barrier, inc=1, device_id={"ja": other}, device_id_type=MESH)
    pl.semaphore_wait(barrier, 2 * (n - 1) + 1)

    def a_plane(r):
        q = plus(ka, r)
        return remote(att.at[pl.ds(pl.multiple_of(q * quart, quart), quart)], a_x.at[ka],
                      sa.at[r - 1], ra.at[r - 1], {"ka": q})

    def a_z(r):
        z = plus(ia, r)
        return remote(a_x.at[z], a_g.at[piece(ia, ka)], sb.at[r - 1], rb_.at[r - 1], {"ia": z})

    def a_spread(b, r):
        rows = a_g.at[piece(minus(ia, b), ka)]
        return remote(rows, rows, sc.at[b, r - 1], rc.at[b, r - 1], {"ka": plus(ka, r)})

    def c_up(d):
        block = c_g.at[ja, span(ia - (d - 1))]
        src = cot if d == 1 else block
        return remote(src, block, su.at[d - 1], ru.at[d - 1], {"ia": ia + 1})

    def c_down(d):
        block = c_g.at[ja, span(ia + (d - 1))]
        src = cot if d == 1 else block
        return remote(src, block, sd.at[d - 1], rd.at[d - 1], {"ia": ia - 1})

    def c_pair_up(d):
        block = c_g.at[ja, span(ia - d)]
        return remote(block, block, spu.at[d - 1], rpu.at[d - 1], {"ja": other})

    def c_pair_down(d):
        block = c_g.at[ja, span(ia + d)]
        return remote(block, block, spd.at[d - 1], rpd.at[d - 1], {"ja": other})

    c_pair_own = remote(cot, c_g.at[ja, span(ia)], spo.at[0], rpo.at[0], {"ja": other})

    def up_exists(d):
        return jnp.logical_and(ia + 1 < n, ia - (d - 1) >= 0)

    def down_exists(d):
        return jnp.logical_and(ia - 1 >= 0, ia + (d - 1) < n)

    def c_step(d):
        @pl.when(ia - d >= 0)
        def _():
            c_up(d).wait_recv()
            if d + 1 < n:
                @pl.when(ia + 1 < n)
                def _():
                    c_up(d + 1).start()
            c_pair_up(d).start()

        @pl.when(ia + d < n)
        def _():
            c_down(d).wait_recv()
            if d + 1 < n:
                @pl.when(ia - 1 >= 0)
                def _():
                    c_down(d + 1).start()
            c_pair_down(d).start()

    w_copy = pltpu.make_async_copy(w_hbm, w, loc.at[0])
    own_x = pltpu.make_async_copy(
        att.at[pl.ds(pl.multiple_of(ka * quart, quart), quart)], a_x.at[ka], loc.at[1])
    own_c = pltpu.make_async_copy(cot, c_g.at[ja, span(ia)], loc.at[2])
    own_a = pltpu.make_async_copy(a_x.at[ia], a_g.at[piece(ia, ka)], loc.at[3])
    for r in range(1, n):
        a_plane(r).start()
    own_x.start()

    c_pair_own.start()
    own_c.start()
    w_copy.start()
    own_x.wait()
    for r in range(1, n):
        a_plane(r).wait_recv()
    for r in range(1, n):
        a_z(r).start()

    @pl.when(up_exists(1))
    def _():
        c_up(1).start()

    @pl.when(down_exists(1))
    def _():
        c_down(1).start()

    own_a.start()
    own_a.wait()
    for r in range(1, n):
        a_spread(0, r).start()

    width = 256

    def i_plane(b, r):
        q = plus(ka, r)
        t = plus(ia, b)
        return remote(i_part.at[piece(t, q)], i_recv.at[b, r - 1],
                      si.at[b, r - 1], ri.at[b, r - 1], {"ka": q})

    def input_block(t):
        @pl.loop(0, rows_w // width)
        def _(c):
            at = pl.multiple_of(c * width, width)
            total = lax.dot_general(
                c_g[0, span(t), :], w[pl.ds(at, width), :half], (((1,), (1,)), ((), ())),
                preferred_element_type=f32)
            total = total + lax.dot_general(
                c_g[1, span(t), :], w[pl.ds(at, width), half:], (((1,), (1,)), ((), ())),
                preferred_element_type=f32)
            i_part[span(t), pl.ds(at, width)] = total.astype(bf16)

    def input_send(b):
        for r in range(1, n):
            i_plane(b, r).start()

    def input_step(d):
        @pl.when(ia - d >= 0)
        def _():
            c_pair_up(d).wait_recv()
            input_block(ia - d)
            input_send(n - d)

        @pl.when(ia + d < n)
        def _():
            c_pair_down(d).wait_recv()
            input_block(ia + d)
            input_send(d)

    w_copy.wait()
    own_c.wait()
    c_pair_own.wait_recv()
    input_block(ia)
    for b in range(1, n):
        a_z(b).wait_recv()
        for r in range(1, n):
            a_spread(b, r).start()
    input_send(0)
    c_step(1)
    input_step(1)
    for b in range(n):
        for r in range(1, n):
            a_spread(b, r).wait_recv()


    def project(which, out):
        @pl.loop(0, half // width)
        def _(c):
            at = pl.multiple_of(which * half + c * width, width)
            to = pl.multiple_of(c * width, width)
            out[:, pl.ds(to, width)] = jnp.dot(
                a_g[...], w[:, pl.ds(at, width)], preferred_element_type=f32
            ).astype(out.dtype)

    def pair(t):
        return remote(p_send.at[pl.ds(t * tok, tok)], p_recv.at[pl.ds(t * tok, tok)],
                      sp.at[t], rp.at[t], {"ja": other})

    project(other, p_send)
    for t in range(n):
        pair(t).start()
    for d in range(2, n - 1):
        c_step(d)
    project(ja, p_own)
    for t in range(n):
        pair(t).wait_recv()

    step_rows = 32

    def add_block(d, out, *incoming):
        @pl.loop(0, tok // step_rows)
        def _(i):
            at = pl.multiple_of(i * step_rows, step_rows)
            mine = pl.ds(d * tok + at, step_rows)
            here = pl.ds(at, step_rows)
            total = p_own[mine, :] + p_recv[mine, :].astype(f32)
            for ref in incoming:
                total = total + ref[here, :].astype(f32)
            out[here, :] = total.astype(bf16)

    def r_up(d):
        return remote(z_buf.at[d], z_up.at[d], sru.at[d], rru.at[d], {"ia": ia + 1})

    def r_down(d):
        return remote(z_buf.at[d], z_dn.at[d], srd.at[d], rrd.at[d], {"ia": ia - 1})

    def reduce_step(tau):
        for m in range(n):
            @pl.when(ia == m)
            def _():
                d = n - 1 - (tau - m)
                if 0 <= tau - m and d > m:
                    if m > 0:
                        r_up(d).wait_recv()
                        add_block(d, z_buf.at[d], z_up.at[d])
                    else:
                        add_block(d, z_buf.at[d])
                    r_up(d).start()
                d = tau - (n - 1 - m)
                if 0 <= d < m:
                    if m < n - 1:
                        r_down(d).wait_recv()
                        add_block(d, z_buf.at[d], z_dn.at[d])
                    else:
                        add_block(d, z_buf.at[d])
                    r_down(d).start()

    reduce_step(0)

    for d in range(2, n - 1):
        input_step(d)
    c_step(n - 1)
    input_step(n - 1)

    def i_to_z(b):
        return remote(i_red.at[b], i_z.at[ia], sz.at[b - 1], rz.at[b - 1], {"ia": plus(ia, b)})

    def i_back(r):
        k = plus(ka, r)
        return remote(i_z.at[k], i_out.at[pl.ds(pl.multiple_of(ka * quart, quart), quart)],
                      so.at[r - 1], ro.at[r - 1], {"ka": k})

    chunks = head // width

    def weight_chunks(first, last):
        @pl.loop(first, last)
        def _(c):
            at = pl.multiple_of(c * width, width)
            lhs = a_g[:, pl.ds(at, width)]
            for j in range(2):
                wg[pl.ds(at, width), j * half:(j + 1) * half] = lax.dot_general(
                    lhs, c_g[j], (((0,), (0,)), ((), ())), preferred_element_type=f32
                ).astype(bf16)

    reduce_step(1)
    weight_chunks(0, chunks // 2)
    for b in range(n):
        for r in range(1, n):
            i_plane(b, r).wait_recv()
        total = i_part[piece(plus(ia, b), ka), :].astype(f32)
        for r in range(1, n):
            total = total + i_recv[b, r - 1].astype(f32)
        if b == 0:
            i_z[ia] = total.astype(bf16)
        else:
            i_red[b] = total.astype(bf16)
            i_to_z(b).start()
    for tau in range(2, n - 1):
        reduce_step(tau)
    weight_chunks(chunks // 2, chunks)
    for b in range(1, n):
        i_to_z(b).wait_recv()
    for r in range(1, n):
        i_back(r).start()
    ig[pl.ds(pl.multiple_of(ka * quart, quart), quart), :] = i_z[ka]
    for m in range(n):
        @pl.when(ia == m)
        def _():
            incoming = []
            if m > 0:
                r_up(m).wait_recv()
                incoming.append(z_up.at[m])
            if m < n - 1:
                r_down(m).wait_recv()
                incoming.append(z_dn.at[m])
            add_block(m, proj, *incoming)
    for r in range(1, n):
        i_back(r).wait_recv()
        rows = pl.ds(pl.multiple_of(minus(ka, r) * quart, quart), quart)
        ig[rows, :] = i_out[rows, :]

    for r in range(1, n):
        a_plane(r).wait_send()
        a_z(r).wait_send()
        i_to_z(r).wait_send()
        i_back(r).wait_send()
        for b in range(n):
            a_spread(b, r).wait_send()
            i_plane(b, r).wait_send()
    c_pair_own.wait_send()
    for t in range(n):
        pair(t).wait_send()
    for d in range(1, n):
        @pl.when(up_exists(d))
        def _():
            c_up(d).wait_send()

        @pl.when(down_exists(d))
        def _():
            c_down(d).wait_send()

        @pl.when(ia - d >= 0)
        def _():
            c_pair_up(d).wait_send()

        @pl.when(ia + d < n)
        def _():
            c_pair_down(d).wait_send()

    for d in range(n):
        @pl.when(ia < d)
        def _():
            r_up(d).wait_send()

        @pl.when(ia > d)
        def _():
            r_down(d).wait_send()


def stationary_weight(n, attended, out_weight, cotangent):
    tok, head = attended.shape
    half = cotangent.shape[1]
    rows = n * tok
    quart = tok // n
    bf16, f32 = jnp.bfloat16, jnp.float32
    vmem = pl.BlockSpec(memory_space=pltpu.VMEM)
    dma = pltpu.SemaphoreType.DMA
    one = dma((n - 1,))
    two = dma((n, n - 1))
    full = dma((n,))
    flops = 6 * rows * out_weight.shape[0] * out_weight.shape[1]
    return pl.pallas_call(
        functools.partial(kernel, n),
        out_shape=(
            jax.ShapeDtypeStruct((tok, half), bf16),
            jax.ShapeDtypeStruct((tok, head), bf16),
            jax.ShapeDtypeStruct(out_weight.shape, bf16),
        ),
        in_specs=[vmem, pl.BlockSpec(memory_space=pl.ANY), vmem],
        out_specs=(vmem, vmem, vmem),
        scratch_shapes=[
            pltpu.VMEM(out_weight.shape, bf16),
            pltpu.VMEM((n, quart, head), bf16),
            pltpu.VMEM((rows, head), bf16),
            pltpu.VMEM((2, rows, half), bf16),
            pltpu.VMEM((rows, half), bf16),
            pltpu.VMEM((rows, half), bf16),
            pltpu.VMEM((rows, half), f32),
            pltpu.VMEM((n, tok, half), bf16),
            pltpu.VMEM((n, tok, half), bf16),
            pltpu.VMEM((n, tok, half), bf16),
            pltpu.VMEM((rows, head), bf16),
            pltpu.VMEM((n, n - 1, quart, head), bf16),
            pltpu.VMEM((n, quart, head), bf16),
            pltpu.VMEM((n, quart, head), bf16),
            pltpu.VMEM((tok, head), bf16),
            full, one, one, one, one, two, two, one, one, one, one,
            one, one, one, one, dma((1,)), dma((1,)),
            full, full, full, full, full, full, two, two, one, one, one, one,
        ],
        compiler_params=pltpu.CompilerParams(
            collective_id=0, has_side_effects=True, vmem_limit_bytes=VMEM_LIMIT
        ),
        cost_estimate=pl.CostEstimate(
            flops=flops, bytes_accessed=6 * rows * half, transcendentals=0
        ),
    )(attended, out_weight, cotangent)


def on_device(sizes, attended, out_weight, cotangent):
    tok, head = attended.shape
    half = cotangent.shape[1]
    n = sizes["ia"]
    tiles = tok % (16 * n) == 0 and head % 256 == 0 and half % 256 == 0
    fits = (
        sizes["ja"] == 2
        and sizes["ka"] == n
        and n >= 3
        and out_weight.shape == (head, 2 * half)
        and head % 512 == 0
        and 4 * out_weight.size + 2 * n * tok * (5 * head + 10 * half) < VMEM_LIMIT
    )
    if tiles and fits:
        return stationary_weight(n, attended, out_weight, cotangent)
    return gathered_weight(attended, out_weight, cotangent)


def solution(mesh):
    return jax.shard_map(
        functools.partial(on_device, dict(mesh.shape)),
        mesh=mesh,
        in_specs=(P("ia", ("ja", "ka")), P(("ja", "ia"), "ka"), P("ia", ("ka", "ja"))),
        out_specs=(P("ia", ("ka", "ja")), P("ia", ("ja", "ka")), P(("ja", "ia"), "ka")),
        check_vma=False,
    )
```

```python
import functools

import jax
import jax.numpy as jnp
from jax import lax
from jax.experimental import pallas as pl
from jax.experimental.pallas import tpu as pltpu
from jax.sharding import PartitionSpec as P

MESH = pl.DeviceIdType.MESH
VMEM_LIMIT = 44 * 1024 * 1024


def gathered_weight(attended, out_weight, cotangent):
    head_rows = lax.all_gather(attended, "ka", axis=1, tiled=True)
    weight_local = lax.all_gather(out_weight, "ia", axis=0, tiled=True)
    partial_value = jnp.dot(head_rows, weight_local, preferred_element_type=jnp.float32)
    projected = lax.psum_scatter(
        partial_value.astype(jnp.bfloat16), "ja", scatter_dimension=1, tiled=True
    )
    grad_rows = lax.all_gather(cotangent, "ja", axis=1, tiled=True)
    input_terms = lax.dot_general(
        grad_rows, weight_local, (((1,), (1,)), ((), ())), preferred_element_type=jnp.float32
    )
    input_grad = lax.psum_scatter(
        input_terms.astype(jnp.bfloat16), "ka", scatter_dimension=1, tiled=True
    )
    weight_terms = lax.dot_general(
        head_rows, grad_rows, (((0,), (0,)), ((), ())), preferred_element_type=jnp.float32
    )
    weight_grad = lax.psum_scatter(
        weight_terms.astype(jnp.bfloat16), "ia", scatter_dimension=0, tiled=True
    )
    return projected, input_grad, weight_grad


def kernel(
    n, att, w_hbm, cot, proj, ig, wg,
    w, a_x, a_g, c_g, p_send, p_recv, p_own, z_buf, z_up, z_dn,
    i_part, i_recv, i_red, i_z, i_out,
    loc, sa, ra, sb, rb_, sc, rc, su, ru, sd, rd, spu, rpu, spd, rpd, spo, rpo,
    sp, rp, sru, rru, srd, rrd, si, ri, sz, rz, so, ro,
):
    ia, ja, ka = lax.axis_index("ia"), lax.axis_index("ja"), lax.axis_index("ka")
    other = 1 - ja
    tok, head = att.shape
    quart = tok // n
    half = cot.shape[1]
    rows_w = w.shape[0]
    f32, bf16 = jnp.float32, jnp.bfloat16

    def plus(x, r):
        return lax.rem(x + r, n)

    def minus(x, r):
        return lax.rem(x + n - r, n)

    def span(t):
        return pl.ds(pl.multiple_of(t * tok, tok), tok)

    def piece(t, q):
        return pl.ds(pl.multiple_of(t * tok + q * quart, quart), quart)

    def remote(src, dst, s, r, where):
        return pltpu.make_async_remote_copy(
            src_ref=src, dst_ref=dst, send_sem=s, recv_sem=r,
            device_id=where, device_id_type=MESH,
        )

    barrier = pltpu.get_barrier_semaphore()
    for r in range(1, n):
        pl.semaphore_signal(barrier, inc=1, device_id={"ka": plus(ka, r)}, device_id_type=MESH)
        pl.semaphore_signal(barrier, inc=1, device_id={"ia": plus(ia, r)}, device_id_type=MESH)
    pl.semaphore_signal(barrier, inc=1, device_id={"ja": other}, device_id_type=MESH)
    pl.semaphore_wait(barrier, 2 * (n - 1) + 1)

    def a_plane(r):
        q = plus(ka, r)
        return remote(att.at[pl.ds(pl.multiple_of(q * quart, quart), quart)], a_x.at[ka],
                      sa.at[r - 1], ra.at[r - 1], {"ka": q})

    def a_z(r):
        z = plus(ia, r)
        return remote(a_x.at[z], a_g.at[piece(ia, ka)], sb.at[r - 1], rb_.at[r - 1], {"ia": z})

    def a_spread(b, r):
        rows = a_g.at[piece(minus(ia, b), ka)]
        return remote(rows, rows, sc.at[b, r - 1], rc.at[b, r - 1], {"ka": plus(ka, r)})

    def c_up(d):
        block = c_g.at[ja, span(ia - (d - 1))]
        src = cot if d == 1 else block
        return remote(src, block, su.at[d - 1], ru.at[d - 1], {"ia": ia + 1})

    def c_down(d):
        block = c_g.at[ja, span(ia + (d - 1))]
        src = cot if d == 1 else block
        return remote(src, block, sd.at[d - 1], rd.at[d - 1], {"ia": ia - 1})

    def c_pair_up(d):
        block = c_g.at[ja, span(ia - d)]
        return remote(block, block, spu.at[d - 1], rpu.at[d - 1], {"ja": other})

    def c_pair_down(d):
        block = c_g.at[ja, span(ia + d)]
        return remote(block, block, spd.at[d - 1], rpd.at[d - 1], {"ja": other})

    c_pair_own = remote(cot, c_g.at[ja, span(ia)], spo.at[0], rpo.at[0], {"ja": other})

    def up_exists(d):
        return jnp.logical_and(ia + 1 < n, ia - (d - 1) >= 0)

    def down_exists(d):
        return jnp.logical_and(ia - 1 >= 0, ia + (d - 1) < n)

    def c_step(d):
        @pl.when(ia - d >= 0)
        def _():
            c_up(d).wait_recv()
            if d + 1 < n:
                @pl.when(ia + 1 < n)
                def _():
                    c_up(d + 1).start()
            c_pair_up(d).start()

        @pl.when(ia + d < n)
        def _():
            c_down(d).wait_recv()
            if d + 1 < n:
                @pl.when(ia - 1 >= 0)
                def _():
                    c_down(d + 1).start()
            c_pair_down(d).start()

    w_copy = pltpu.make_async_copy(w_hbm, w, loc.at[0])
    own_x = pltpu.make_async_copy(
        att.at[pl.ds(pl.multiple_of(ka * quart, quart), quart)], a_x.at[ka], loc.at[1])
    own_c = pltpu.make_async_copy(cot, c_g.at[ja, span(ia)], loc.at[2])
    own_a = pltpu.make_async_copy(a_x.at[ia], a_g.at[piece(ia, ka)], loc.at[3])
    for r in range(1, n):
        a_plane(r).start()
    own_x.start()

    c_pair_own.start()
    own_c.start()
    w_copy.start()
    own_x.wait()
    for r in range(1, n):
        a_plane(r).wait_recv()
    for r in range(1, n):
        a_z(r).start()

    @pl.when(up_exists(1))
    def _():
        c_up(1).start()

    @pl.when(down_exists(1))
    def _():
        c_down(1).start()

    own_a.start()
    own_a.wait()
    for r in range(1, n):
        a_spread(0, r).start()

    width = 256

    def i_plane(b, r):
        q = plus(ka, r)
        t = plus(ia, b)
        return remote(i_part.at[piece(t, q)], i_recv.at[b, r - 1],
                      si.at[b, r - 1], ri.at[b, r - 1], {"ka": q})

    def input_block(t):
        @pl.loop(0, rows_w // width)
        def _(c):
            at = pl.multiple_of(c * width, width)
            total = lax.dot_general(
                c_g[0, span(t), :], w[pl.ds(at, width), :half], (((1,), (1,)), ((), ())),
                preferred_element_type=f32)
            total = total + lax.dot_general(
                c_g[1, span(t), :], w[pl.ds(at, width), half:], (((1,), (1,)), ((), ())),
                preferred_element_type=f32)
            i_part[span(t), pl.ds(at, width)] = total.astype(bf16)

    def input_send(b):
        for r in range(1, n):
            i_plane(b, r).start()

    def input_step(d):
        @pl.when(ia - d >= 0)
        def _():
            c_pair_up(d).wait_recv()
            input_block(ia - d)
            input_send(n - d)

        @pl.when(ia + d < n)
        def _():
            c_pair_down(d).wait_recv()
            input_block(ia + d)
            input_send(d)

    w_copy.wait()
    own_c.wait()
    c_pair_own.wait_recv()
    input_block(ia)
    for b in range(1, n):
        a_z(b).wait_recv()
        for r in range(1, n):
            a_spread(b, r).start()
    input_send(0)
    c_step(1)
    input_step(1)
    for b in range(n):
        for r in range(1, n):
            a_spread(b, r).wait_recv()


    def project(which, out):
        @pl.loop(0, half // width)
        def _(c):
            at = pl.multiple_of(which * half + c * width, width)
            to = pl.multiple_of(c * width, width)
            out[:, pl.ds(to, width)] = jnp.dot(
                a_g[...], w[:, pl.ds(at, width)], preferred_element_type=f32
            ).astype(out.dtype)

    def pair(t):
        return remote(p_send.at[pl.ds(t * tok, tok)], p_recv.at[pl.ds(t * tok, tok)],
                      sp.at[t], rp.at[t], {"ja": other})

    project(other, p_send)
    for t in range(n):
        pair(t).start()
    for d in range(2, n - 1):
        c_step(d)
    project(ja, p_own)
    for t in range(n):
        pair(t).wait_recv()

    step_rows = 32

    def add_block(d, out, *incoming):
        @pl.loop(0, tok // step_rows)
        def _(i):
            at = pl.multiple_of(i * step_rows, step_rows)
            mine = pl.ds(d * tok + at, step_rows)
            here = pl.ds(at, step_rows)
            total = p_own[mine, :] + p_recv[mine, :].astype(f32)
            for ref in incoming:
                total = total + ref[here, :].astype(f32)
            out[here, :] = total.astype(bf16)

    def r_up(d):
        return remote(z_buf.at[d], z_up.at[d], sru.at[d], rru.at[d], {"ia": ia + 1})

    def r_down(d):
        return remote(z_buf.at[d], z_dn.at[d], srd.at[d], rrd.at[d], {"ia": ia - 1})

    def reduce_step(tau):
        for m in range(n):
            @pl.when(ia == m)
            def _():
                if m == 0 and tau == 0:
                    for d in range(n - 1, 0, -1):
                        add_block(d, z_buf.at[d])
                        r_up(d).start()
                d = n - 1 - (tau - m)
                if m > 0 and tau >= m and d > m:
                    r_up(d).wait_recv()
                    add_block(d, z_buf.at[d], z_up.at[d])
                    r_up(d).start()
                if m == n - 1 and tau == 0:
                    for d in range(n - 1):
                        add_block(d, z_buf.at[d])
                        r_down(d).start()
                d = tau - (n - 1 - m)
                if m < n - 1 and 0 <= d < m:
                    r_down(d).wait_recv()
                    add_block(d, z_buf.at[d], z_dn.at[d])
                    r_down(d).start()

    reduce_step(0)

    for d in range(2, n - 1):
        input_step(d)
    c_step(n - 1)
    input_step(n - 1)

    def i_to_z(b):
        return remote(i_red.at[b], i_z.at[ia], sz.at[b - 1], rz.at[b - 1], {"ia": plus(ia, b)})

    def i_back(r):
        k = plus(ka, r)
        return remote(i_z.at[k], i_out.at[pl.ds(pl.multiple_of(ka * quart, quart), quart)],
                      so.at[r - 1], ro.at[r - 1], {"ka": k})

    chunks = head // width

    def weight_chunks(first, last):
        @pl.loop(first, last)
        def _(c):
            at = pl.multiple_of(c * width, width)
            lhs = a_g[:, pl.ds(at, width)]
            for j in range(2):
                wg[pl.ds(at, width), j * half:(j + 1) * half] = lax.dot_general(
                    lhs, c_g[j], (((0,), (0,)), ((), ())), preferred_element_type=f32
                ).astype(bf16)

    reduce_step(1)
    weight_chunks(0, chunks // 2)
    for b in range(n):
        for r in range(1, n):
            i_plane(b, r).wait_recv()
        total = i_part[piece(plus(ia, b), ka), :].astype(f32)
        for r in range(1, n):
            total = total + i_recv[b, r - 1].astype(f32)
        if b == 0:
            i_z[ia] = total.astype(bf16)
        else:
            i_red[b] = total.astype(bf16)
            i_to_z(b).start()
    for tau in range(2, n - 1):
        reduce_step(tau)
    weight_chunks(chunks // 2, chunks)
    for b in range(1, n):
        i_to_z(b).wait_recv()
    for r in range(1, n):
        i_back(r).start()
    ig[pl.ds(pl.multiple_of(ka * quart, quart), quart), :] = i_z[ka]
    for m in range(n):
        @pl.when(ia == m)
        def _():
            incoming = []
            if m > 0:
                r_up(m).wait_recv()
                incoming.append(z_up.at[m])
            if m < n - 1:
                r_down(m).wait_recv()
                incoming.append(z_dn.at[m])
            add_block(m, proj, *incoming)
    for r in range(1, n):
        i_back(r).wait_recv()
        rows = pl.ds(pl.multiple_of(minus(ka, r) * quart, quart), quart)
        ig[rows, :] = i_out[rows, :]

    for r in range(1, n):
        a_plane(r).wait_send()
        a_z(r).wait_send()
        i_to_z(r).wait_send()
        i_back(r).wait_send()
        for b in range(n):
            a_spread(b, r).wait_send()
            i_plane(b, r).wait_send()
    c_pair_own.wait_send()
    for t in range(n):
        pair(t).wait_send()
    for d in range(1, n):
        @pl.when(up_exists(d))
        def _():
            c_up(d).wait_send()

        @pl.when(down_exists(d))
        def _():
            c_down(d).wait_send()

        @pl.when(ia - d >= 0)
        def _():
            c_pair_up(d).wait_send()

        @pl.when(ia + d < n)
        def _():
            c_pair_down(d).wait_send()

    for d in range(n):
        @pl.when(ia < d)
        def _():
            r_up(d).wait_send()

        @pl.when(ia > d)
        def _():
            r_down(d).wait_send()


def stationary_weight(n, attended, out_weight, cotangent):
    tok, head = attended.shape
    half = cotangent.shape[1]
    rows = n * tok
    quart = tok // n
    bf16, f32 = jnp.bfloat16, jnp.float32
    vmem = pl.BlockSpec(memory_space=pltpu.VMEM)
    dma = pltpu.SemaphoreType.DMA
    one = dma((n - 1,))
    two = dma((n, n - 1))
    full = dma((n,))
    flops = 6 * rows * out_weight.shape[0] * out_weight.shape[1]
    return pl.pallas_call(
        functools.partial(kernel, n),
        out_shape=(
            jax.ShapeDtypeStruct((tok, half), bf16),
            jax.ShapeDtypeStruct((tok, head), bf16),
            jax.ShapeDtypeStruct(out_weight.shape, bf16),
        ),
        in_specs=[vmem, pl.BlockSpec(memory_space=pl.ANY), vmem],
        out_specs=(vmem, vmem, vmem),
        scratch_shapes=[
            pltpu.VMEM(out_weight.shape, bf16),
            pltpu.VMEM((n, quart, head), bf16),
            pltpu.VMEM((rows, head), bf16),
            pltpu.VMEM((2, rows, half), bf16),
            pltpu.VMEM((rows, half), bf16),
            pltpu.VMEM((rows, half), bf16),
            pltpu.VMEM((rows, half), f32),
            pltpu.VMEM((n, tok, half), bf16),
            pltpu.VMEM((n, tok, half), bf16),
            pltpu.VMEM((n, tok, half), bf16),
            pltpu.VMEM((rows, head), bf16),
            pltpu.VMEM((n, n - 1, quart, head), bf16),
            pltpu.VMEM((n, quart, head), bf16),
            pltpu.VMEM((n, quart, head), bf16),
            pltpu.VMEM((tok, head), bf16),
            full, one, one, one, one, two, two, one, one, one, one,
            one, one, one, one, dma((1,)), dma((1,)),
            full, full, full, full, full, full, two, two, one, one, one, one,
        ],
        compiler_params=pltpu.CompilerParams(
            collective_id=0, has_side_effects=True, vmem_limit_bytes=VMEM_LIMIT
        ),
        cost_estimate=pl.CostEstimate(
            flops=flops, bytes_accessed=6 * rows * half, transcendentals=0
        ),
    )(attended, out_weight, cotangent)


def on_device(sizes, attended, out_weight, cotangent):
    tok, head = attended.shape
    half = cotangent.shape[1]
    n = sizes["ia"]
    tiles = tok % (16 * n) == 0 and head % 256 == 0 and half % 256 == 0
    fits = (
        sizes["ja"] == 2
        and sizes["ka"] == n
        and n >= 3
        and out_weight.shape == (head, 2 * half)
        and head % 512 == 0
        and 4 * out_weight.size + 2 * n * tok * (5 * head + 10 * half) < VMEM_LIMIT
    )
    if tiles and fits:
        return stationary_weight(n, attended, out_weight, cotangent)
    return gathered_weight(attended, out_weight, cotangent)


def solution(mesh):
    return jax.shard_map(
        functools.partial(on_device, dict(mesh.shape)),
        mesh=mesh,
        in_specs=(P("ia", ("ja", "ka")), P(("ja", "ia"), "ka"), P("ia", ("ka", "ja"))),
        out_specs=(P("ia", ("ka", "ja")), P("ia", ("ja", "ka")), P(("ja", "ia"), "ka")),
        check_vma=False,
    )
```
